32 devices in a mesh: row: 4 (over z), col: 4 (over x, core), layer: 2 (over y).
Axes of the slice: x: 2, y: 2, z: 4, core: 2. Of those that a mesh axis runs over, the one named last changes fastest.
Arguments:
- left: bfloat16 [4096, 8192], P('row', ('col', 'layer')), may hold values from -6 to 6
- middle: bfloat16 [8192, 8192], P('row', 'col'), may hold values from -0.0625 to 0.0625
- right: bfloat16 [8192, 8192], P('row', 'col'), may hold values from -0.0625 to 0.0625
Outputs:
- product: bfloat16 [4096, 8192], P('row', ('col', 'layer'))
The draws below stay inside these ranges and needn't reach their ends.
All inputs are finite; a program needn't handle non-finite values.
Results may differ from the reference program's by a relative error of at most 0.0049.
Values may be sent and summed in bfloat16 or wider, within the bound.
A program may use at most 128 MiB of HBM per device.

```python
import jax
import jax.numpy as jnp

K = 8192
N = 8192
P_SIZE = 8192
M = 4096


def block_scale(rng, dims, pieces, low, high):
    loudness, own = 1.0, jax.random.fold_in(rng, 6)
    for axis_at, shards_of in pieces:
        heights = jnp.exp(jax.random.uniform(jax.random.fold_in(own, axis_at), (shards_of,), jnp.float32, low / len(pieces), high / len(pieces)))
        loudness = loudness * jnp.repeat(heights, dims[axis_at] // shards_of).reshape([-1 if axis == axis_at else 1 for axis in range(len(dims))])
    return loudness


def scatter_about(key, dims, deviation, limit, shards=(), kind=jnp.bfloat16):
    array = jax.random.normal(key, dims, jnp.float32) * deviation
    if len(shards) > 0:
        array = block_scale(key, dims, shards, -0.22, 0.18) * array
    return jnp.clip(array, min=-limit, max=limit).astype(kind)


def setup_inputs(seed: int = 0) -> dict:
    streams_of = jax.random.split(jax.random.key(seed), 4)
    return {
        "left": scatter_about(streams_of[0], (M, K), 1.0, 6.0, ((0, 4), (1, 8))),
        "middle": scatter_about(streams_of[1], (K, N), K ** -0.5, 0.0625, ((0, 4), (1, 4))),
        "right": scatter_about(streams_of[2], (N, P_SIZE), N ** -0.5, 0.0625, ((0, 4), (1, 4))),
    }


def reference(left, middle, right):
    first = jnp.dot(left, middle, preferred_element_type=jnp.float32).astype(jnp.bfloat16)
    return jnp.dot(first, right, preferred_element_type=jnp.float32).astype(jnp.bfloat16)
```

```python
import functools

import jax
import jax.numpy as jnp
from jax import lax
from jax.experimental import pallas as pl
from jax.experimental.pallas import tpu as pltpu
from jax.sharding import PartitionSpec as P

CHUNKS = 4
TILE = 256
MESH = pl.DeviceIdType.MESH


def kernel(
    rows, cols, layers,
    left_ref, middle_ref, right_ref, out_ref,
    held, held2, rhs, sent, kept, near, far, near2,
    own_sem, home_sem, swap_sems, pair_sems, plane_sems, core_sems, near_sems, far_sems, near2_sems,
):
    group, side = rows // 2, cols // 2
    row, col, layer = lax.axis_index("row"), lax.axis_index("col"), lax.axis_index("layer")
    h, z = row // group, lax.rem(row, group)
    x, c = col // side, lax.rem(col, side)
    straight = h == x
    depth = middle_ref.shape[0]
    width = out_ref.shape[1]
    inner = left_ref.shape[1]
    chunk = left_ref.shape[0] // CHUNKS
    tile = min(TILE, width)

    def at(h_, x_):
        return (h_ * group + z, x_ * side + c, layer)

    def slot(col_, layer_):
        return col_ * layers + layer_

    sibling = col + 1 - 2 * lax.rem(col, 2)
    offsets = [(dc, dl) for dc in range(cols // 2) for dl in range(layers) if dc or dl]

    def moved(col_, dc, dl, sign):
        return lax.rem(col_ + sign * 2 * dc + cols, cols), lax.rem(layer + sign * dl + layers, layers)

    barrier = pltpu.get_barrier_semaphore()
    greeted = [at(1 - h, x), at(h, 1 - x), at(1 - h, 1 - x), (row, sibling, layer)]
    for shift in range(1, group):
        greeted.append((h * group + lax.rem(z + shift, group), col, layer))
    for dc, dl in offsets:
        greeted.append((row, *moved(col, dc, dl, 1)))
    for device in greeted:
        pl.semaphore_signal(barrier, inc=1, device_id=device, device_id_type=MESH)
    pl.semaphore_wait(barrier, len(greeted))

    me = slot(col, layer)

    def part(j):
        return pl.ds(j * chunk, chunk)

    def remote(src, dst, sems, device):
        return pltpu.make_async_remote_copy(
            src_ref=src, dst_ref=dst, send_sem=sems.at[0], recv_sem=sems.at[1],
            device_id=device, device_id_type=MESH,
        )

    home = pltpu.make_async_copy(left_ref, held.at[me], home_sem)

    def swap(j):
        return remote(
            left_ref.at[part(j)], held.at[slot(h * side + c, layer), part(j)],
            swap_sems.at[j], at(x, h),
        )

    columns = pl.ds(pl.multiple_of(layer * width, width), width)
    pieces = CHUNKS
    step = depth // pieces

    def own(which):
        ref = (middle_ref, right_ref)[which]
        return pltpu.make_async_copy(
            ref.at[:, columns], rhs.at[which, pl.ds(z * depth, depth)], own_sem.at[which]
        )

    def pair(which, piece, shift):
        ref = (middle_ref, right_ref)[which]
        return remote(
            ref.at[pl.ds(piece * step, step), columns],
            rhs.at[which, pl.ds(z * depth + piece * step, step)],
            pair_sems.at[which, piece, shift - 1],
            (h * group + lax.rem(z + shift, group), col, layer),
        )

    def pair_start(which, piece):
        for shift in range(1, group):
            pair(which, piece, shift).start()

    def pair_wait(which):
        for piece in range(pieces):
            for shift in range(1, group):
                pair(which, piece, shift).wait_recv()
        own(which).wait()

    buffers = (held, held2)

    def spread(phase, j, index):
        dc, dl = offsets[index]
        ref = buffers[phase].at[me, part(j)]
        return remote(ref, ref, plane_sems.at[phase, j, index], (row, *moved(col, dc, dl, 1)))

    def pass_on(phase, j, index):
        origin = me
        if index:
            dc, dl = offsets[index - 1]
            origin = slot(*moved(col, dc, dl, -1))
        ref = buffers[phase].at[origin, part(j)]
        return remote(ref, ref, core_sems.at[phase, j, index], (row, sibling, layer))

    def spread_start(phase, j):
        for index in range(len(offsets)):
            spread(phase, j, index).start()
        pass_on(phase, j, 0).start()

    def spread_finish(phase, j):
        for index in range(len(offsets)):
            spread(phase, j, index).wait_recv()
            pass_on(phase, j, index + 1).start()
        for index in range(len(offsets) + 1):
            pass_on(phase, j, index).wait_recv()

    def multiply(phase, j, piece, target):
        blocks = side * layers
        ref = buffers[phase]

        @pl.loop(0, width // tile)
        def _(n):
            across = pl.ds(pl.multiple_of(n * tile, tile), tile)
            total = jnp.zeros((chunk, tile), jnp.float32)
            for k in range(blocks):
                total += jnp.dot(
                    ref[piece * blocks + k, part(j), :],
                    rhs[phase, pl.ds(k * inner, inner), across],
                    preferred_element_type=jnp.float32,
                )
            target[part(j), across] = total.astype(target.dtype)

    def add(one, two, j, store):
        @pl.loop(0, chunk // 32)
        def _(i):
            span = pl.ds(pl.multiple_of(j * chunk + i * 32, 32), 32)
            value = one[span, :].astype(jnp.float32) + two[span, :].astype(jnp.float32)
            store(span, value.astype(jnp.bfloat16))

    def near_copy(j):
        target_row = jnp.where(straight, h, x)
        target_col = jnp.where(straight, 1 - x, x)
        return remote(sent.at[part(j)], near.at[part(j)], near_sems.at[j], at(target_row, target_col))

    def far_copy(j):
        return remote(kept.at[part(j)], far.at[part(j)], far_sems.at[j], at(x, 1 - x))

    def near2_copy(j):
        return remote(sent.at[part(j)], near2.at[part(j)], near2_sems.at[j], at(1 - h, x))

    @pl.when(straight)
    def _():
        home.start()

    @pl.when(jnp.logical_not(straight))
    def _():
        for j in range(CHUNKS):
            swap(j).start()

    own(0).start()
    own(1).start()
    for piece in range(pieces):
        pair_start(0, piece)

    @pl.when(straight)
    def _():
        home.wait()

    for j in range(CHUNKS):
        @pl.when(jnp.logical_not(straight))
        def _():
            swap(j).wait_recv()

        spread_start(0, j)

    def first_done(j):
        near_copy(j).wait_recv()

        def store(span, value):
            held2[me, span, :] = value

        @pl.when(straight)
        def _():
            add(near, kept, j, store)

        @pl.when(jnp.logical_not(straight))
        def _():
            far_copy(j).wait_recv()
            add(near, far, j, store)

        spread_start(1, j)

    for j in range(CHUNKS):
        spread_finish(0, j)
        if j == 0:
            pair_wait(0)
        multiply(0, j, 1 - h, sent)
        near_copy(j).start()
        multiply(0, j, h, kept)

        @pl.when(jnp.logical_not(straight))
        def _():
            far_copy(j).start()

        pair_start(1, j)
        if j:
            first_done(j - 1)
    first_done(CHUNKS - 1)

    def out_done(j):
        near2_copy(j).wait_recv()

        def store(span, value):
            out_ref[span, :] = value

        add(near2, kept, j, store)

    for j in range(CHUNKS):
        spread_finish(1, j)
        if j == 0:
            pair_wait(1)
        near_copy(j).wait_send()

        @pl.when(jnp.logical_not(straight))
        def _():
            far_copy(j).wait_send()

        multiply(1, j, 1 - h, sent)
        near2_copy(j).start()
        multiply(1, j, h, kept)
        if j:
            out_done(j - 1)
    out_done(CHUNKS - 1)

    @pl.when(jnp.logical_not(straight))
    def _():
        for j in range(CHUNKS):
            swap(j).wait_send()

    for j in range(CHUNKS):
        near2_copy(j).wait_send()
        for phase in range(2):
            for index in range(len(offsets)):
                spread(phase, j, index).wait_send()
            for index in range(len(offsets) + 1):
                pass_on(phase, j, index).wait_send()
    for which in range(2):
        for piece in range(pieces):
            for shift in range(1, group):
                pair(which, piece, shift).wait_send()


def per_device(left, middle, right):
    rows, cols, layers = (lax.axis_size(name) for name in ("row", "col", "layer"))
    height, inner = left.shape
    width = right.shape[1] // layers
    depth = right.shape[0]
    group = rows // 2
    partners = cols // 2 * layers - 1
    bf16 = jnp.bfloat16
    anywhere = pl.BlockSpec(memory_space=pl.ANY)
    dma = pltpu.SemaphoreType.DMA
    return pl.pallas_call(
        functools.partial(kernel, rows, cols, layers),
        out_shape=jax.ShapeDtypeStruct((height, width), bf16),
        in_specs=[anywhere] * 3,
        out_specs=pl.BlockSpec(memory_space=pltpu.VMEM),
        scratch_shapes=[
            pltpu.VMEM((cols * layers, height, inner), bf16),
            pltpu.VMEM((cols * layers, height, inner), bf16),
            pltpu.VMEM((2, group * depth, width), bf16),
        ]
        + [pltpu.VMEM((height, width), bf16)] * 5
        + [
            dma((2,)),
            dma,
            dma((CHUNKS, 2)),
            dma((2, CHUNKS, max(group - 1, 1), 2)),
            dma((2, CHUNKS, partners, 2)),
            dma((2, CHUNKS, partners + 1, 2)),
            dma((CHUNKS, 2)),
            dma((CHUNKS, 2)),
            dma((CHUNKS, 2)),
        ],
        compiler_params=pltpu.CompilerParams(
            collective_id=0, has_side_effects=True, vmem_limit_bytes=67043328
        ),
    )(left, middle, right)


def solution(mesh):
    return jax.shard_map(
        per_device,
        mesh=mesh,
        in_specs=(P("row", ("col", "layer")), P("row", "col"), P("row", "col")),
        out_specs=P("row", ("col", "layer")),
        check_vma=False,
    )
```
